32 devices in a mesh: replica: 1 (over z), data2: 4 (over y), data: 8 (over x, core).
Axes of the slice: x: 4, y: 4, z: 1, core: 2. Of those that a mesh axis runs over, the one named last changes fastest.
The devices are a block of a 4x4x8 slice.
Arguments:
- query_hidden: bfloat16 [256, 32, 1024], P(('replica', 'data2', 'data'))
- doc_hidden: bfloat16 [256, 512, 1024], P(('replica', 'data2', 'data'))
- w_proj: bfloat16 [1024, 128], replicated
- query_mask: int32 [256, 32], P(('replica', 'data2', 'data'))
- doc_mask: int32 [256, 512], P(('replica', 'data2', 'data'))
- temperature: float32 [], replicated
Outputs:
- output 1: float32 [256], P(('replica', 'data2', 'data'))
- output 2: float32 [1], P('replica')
All inputs are finite; a program needn't handle non-finite values.
Results may differ from the reference program's by a relative error of at most 0.001.
Values are sent between devices in bfloat16 or wider.
A program may use at most 768 MiB of HBM per device.

```python
import jax
import jax.numpy as jnp
from jax import lax

BATCH = 256
QLEN = 32
DLEN = 512
HIDDEN = 1024
PROJ = 128


def setup_inputs(seed: int = 0, part: int = 0) -> dict:
    root_key = jax.random.key(seed)
    key_common, key_parts = jax.random.split(root_key)
    part_key = jax.random.fold_in(key_parts, part)
    key_list = jax.random.split(part_key, 6)
    key_weight, key_temp = jax.random.split(key_common)
    shared = jax.random.normal(key_list[0], (HIDDEN,), jnp.float32)
    topic_vec = jax.random.normal(key_list[1], (BATCH, 1, HIDDEN), jnp.float32)
    concept = jax.random.normal(key_list[2], (BATCH, QLEN, HIDDEN), jnp.float32)
    token_noise = jax.random.normal(key_list[3], (BATCH, DLEN, HIDDEN), jnp.float32)
    query_lens = jax.random.randint(key_list[4], (BATCH,), QLEN // 2, QLEN + 1)
    doc_lens = jax.random.randint(key_list[5], (BATCH,), DLEN // 4, DLEN + 1)
    query_mask = (jnp.arange(QLEN)[None, :] < query_lens[:, None]).astype(jnp.int32)
    doc_mask = (jnp.arange(DLEN)[None, :] < doc_lens[:, None]).astype(jnp.int32)
    base_state = 0.6 * shared + 0.6 * topic_vec
    query_hidden = base_state + concept
    doc_concept = jnp.take(concept, jnp.arange(DLEN) % QLEN, axis=1)
    real_tok = base_state + 0.6 * doc_concept + 0.8 * token_noise
    pad_tok = 1.5 * shared + token_noise
    doc_hidden = jnp.where(doc_mask[:, :, None] > 0, real_tok, pad_tok)
    w_proj = jax.random.normal(key_weight, (HIDDEN, PROJ), jnp.float32) * HIDDEN ** -0.5
    temperature = QLEN * jax.random.uniform(key_temp, (), jnp.float32, 0.8, 1.25) / 8.0
    return {'query_hidden': query_hidden.astype(jnp.bfloat16), 'doc_hidden': doc_hidden.astype(jnp.bfloat16), 'w_proj': w_proj.astype(jnp.bfloat16), 'query_mask': query_mask, 'doc_mask': doc_mask, 'temperature': temperature}


def project_norm(hidden, w_proj):
    flat_states = hidden.reshape(-1, HIDDEN)
    projected = jnp.dot(flat_states, w_proj, preferred_element_type=jnp.float32)
    norm_len = jnp.sqrt(jnp.sum(projected * projected, axis=-1, keepdims=True))
    unit_vecs = projected / jnp.maximum(norm_len, 1e-12)
    return unit_vecs.astype(jnp.bfloat16).reshape(hidden.shape[0], hidden.shape[1], PROJ)


def reference(query_hidden, doc_hidden, w_proj, query_mask, doc_mask, temperature):
    q_vecs = project_norm(query_hidden, w_proj)
    p_vecs = project_norm(doc_hidden, w_proj).astype(jnp.float32)
    doc_valid = doc_mask[None, :, :] > 0

    def query_row(query_args):
        q_tok, q_weight = query_args
        similarity = jnp.einsum('tc,jsc->tjs', q_tok.astype(jnp.float32), p_vecs)
        best_match = jnp.max(jnp.where(doc_valid, similarity, -jnp.inf), axis=-1)
        return jnp.sum(q_weight.astype(jnp.float32)[:, None] * best_match, axis=0)

    scores = lax.map(query_row, (q_vecs, query_mask))
    logits = scores / temperature
    losses = jax.nn.logsumexp(logits, axis=1) - jnp.diagonal(logits)
    mean_loss = jnp.mean(losses).reshape(1)
    return losses, mean_loss
```

```python
import functools

import jax
import jax.numpy as jnp
from jax import lax
from jax.experimental import pallas as pl
from jax.experimental.pallas import tpu as pltpu
from jax.sharding import PartitionSpec as P

MESH = pl.DeviceIdType.MESH
CORES = 2
LANES = 128
MASKED = -1e30
DOC_CHUNKS = 4


def unit_rows(hidden, w_proj):
    projected = jnp.dot(hidden, w_proj, preferred_element_type=jnp.float32)
    square = jnp.sum(projected * projected, axis=-1, keepdims=True)
    return projected * lax.rsqrt(jnp.maximum(square, 1e-24))


def kernel(outer, inner, pairs, qlen, dlen,
           hq_hbm, doc_hbm, w_hbm, qm_hbm, dm_hbm, temp_ref, loss_ref, mean_ref,
           hq, doc, w, qm, dm, qall, paug, best, xout, xin,
           load_sem, doc_sem, send_sem, relay_sem, recv_sem, xsend_sem, xrecv_sem):
    devices = outer * inner
    columns = inner // CORES
    chips = outer * columns
    tokens = pairs * qlen
    width = w.shape[1]
    rows = doc.shape[0] // DOC_CHUNKS
    per_half = LANES // pairs
    halves = devices // per_half
    y, d = lax.axis_index('data2'), lax.axis_index('data')
    x, core = d // CORES, d % CORES
    me = y * inner + d
    partner = {'data2': y, 'data': x * CORES + 1 - core}

    loads = [pltpu.make_async_copy(src, dst, load_sem.at[k])
             for k, (src, dst) in enumerate(((w_hbm, w), (hq_hbm, hq), (qm_hbm, qm), (dm_hbm, dm)))]
    for load in loads:
        load.start()
    doc_loads = []
    for k in range(DOC_CHUNKS):
        part = pl.ds(k * rows, rows)
        doc_loads.append(pltpu.make_async_copy(doc_hbm.at[part], doc.at[part], doc_sem.at[k]))
        doc_loads[-1].start()

    barrier = pltpu.get_barrier_semaphore()
    for k in range(1, devices):
        there = {'data2': (y + k // inner) % outer, 'data': (d + k % inner) % inner}
        pl.semaphore_signal(barrier, inc=1, device_id=there, device_id_type=MESH)

    ones = (lax.broadcasted_iota(jnp.int32, (width, tokens), 0) < pairs).astype(jnp.float32).astype(jnp.bfloat16)

    @pl.loop(0, devices)
    def _(slot):
        qall[slot, width:, :] = ones

    loads[3].wait()
    bias = jnp.where(dm[...] > 0, 0.0, MASKED)
    bias = jnp.concatenate([bias, jnp.zeros((LANES - pairs, dlen), jnp.float32)], axis=0).T
    lane = lax.broadcasted_iota(jnp.int32, (dlen, LANES), 1)
    for j in range(pairs):
        paug[j * dlen:(j + 1) * dlen, width:] = jnp.where(lane == j, bias, 0.0).astype(jnp.bfloat16)

    for load in loads[:3]:
        load.wait()
    spread = (lax.broadcasted_iota(jnp.int32, (qlen, tokens), 1) % qlen
              == lax.broadcasted_iota(jnp.int32, (qlen, tokens), 0)).astype(jnp.float32).astype(jnp.bfloat16)
    keep = jnp.dot(qm[...].astype(jnp.float32).astype(jnp.bfloat16), spread, preferred_element_type=jnp.float32)
    own = (lax.broadcasted_iota(jnp.int32, (pairs, tokens), 1) // qlen
           == lax.broadcasted_iota(jnp.int32, (pairs, tokens), 0))
    keep = jnp.sum(jnp.where(own, keep, 0.0), axis=0, keepdims=True)
    q_t = unit_rows(hq[...], w[...]).T
    qall[me, :width, :] = jnp.where(keep > 0, q_t, 0.0).astype(jnp.bfloat16)

    def source(i, other):
        row = (y + outer - i // columns) % outer
        column = (x + columns - i % columns) % columns
        return row * inner + column * CORES + (1 - core if other else core)

    def block_copy(slot, sem, there):
        block = qall.at[slot, pl.ds(0, width), :]
        return pltpu.make_async_remote_copy(
            src_ref=block, dst_ref=block, send_sem=sem, recv_sem=recv_sem.at[slot],
            device_id=there, device_id_type=MESH)

    pl.semaphore_wait(barrier, devices - 1)
    sends = [block_copy(me, relay_sem.at[0], partner)]
    for i in range(1, chips):
        there = {'data2': (y + i // columns) % outer, 'data': (x + i % columns) % columns * CORES + core}
        sends.append(block_copy(me, send_sem.at[i], there))
    for send in sends:
        send.start()

    for k in range(DOC_CHUNKS):
        doc_loads[k].wait()
        part = pl.ds(k * rows, rows)
        paug[part, :width] = unit_rows(doc[part, :], w[...]).astype(jnp.bfloat16)

    def score(slot):
        for j in range(pairs):
            similarity = jnp.dot(paug[j * dlen:(j + 1) * dlen, :], qall[slot], preferred_element_type=jnp.float32)
            similarity = jnp.max(similarity.reshape(4, dlen // 32, 8, tokens), axis=1)
            best[slot, j:j + 1, :] = jnp.max(jnp.max(similarity, axis=0), axis=0, keepdims=True)

    @pl.loop(0, chips)
    def _(i):
        @pl.when(i + 1 < chips)
        def _():
            arrived = source(i + 1, False)
            block_copy(arrived, relay_sem.at[i + 1], partner).wait_recv()
            block_copy(arrived, relay_sem.at[i + 1], partner).start()

        relayed = source(i, True)
        block_copy(relayed, relay_sem.at[i], partner).wait_recv()
        score(source(i, False))
        score(relayed)

    pick = (lax.broadcasted_iota(jnp.int32, (tokens, LANES), 0) // qlen
            == lax.broadcasted_iota(jnp.int32, (tokens, LANES), 1) % pairs).astype(jnp.float32).astype(jnp.bfloat16)
    rest = best[...].reshape(devices * pairs, tokens)
    sums = jnp.zeros((devices * pairs, LANES), jnp.float32)
    for _ in range(3):
        part = rest.astype(jnp.bfloat16)
        sums += jnp.dot(part, pick, preferred_element_type=jnp.float32)
        rest = rest - part.astype(jnp.float32)
    sums = sums.reshape(devices, pairs, LANES)
    lane = lax.broadcasted_iota(jnp.int32, (pairs, LANES), 1)
    own_doc = lane % pairs == lax.broadcasted_iota(jnp.int32, (pairs, LANES), 0)
    temperature = temp_ref[0]
    own_row = jnp.zeros((1, LANES), jnp.float32)
    for h in range(halves):
        logits = jnp.zeros((pairs, LANES), jnp.float32)
        for b in range(per_half):
            logits = jnp.where(lane // pairs == b, sums[h * per_half + b], logits)
        logits = logits / temperature
        top = jnp.max(logits, axis=0, keepdims=True)
        xout[h:h + 1, :] = top + jnp.log(jnp.sum(jnp.exp(logits - top), axis=0, keepdims=True))
        mine = own_doc & (h * per_half + lane // pairs == me)
        own_row += jnp.sum(jnp.where(mine, logits, 0.0), axis=0, keepdims=True)
    xout[halves:halves + 1, :] = own_row
    for h in range(halves + 1, xout.shape[0]):
        xout[h:h + 1, :] = jnp.zeros((1, LANES), jnp.float32)
    xin[me] = xout[...]

    shares = []
    for k in range(1, devices):
        there = {'data2': (y + k // inner) % outer, 'data': (d + k % inner) % inner}
        shares.append(pltpu.make_async_remote_copy(
            src_ref=xout, dst_ref=xin.at[me], send_sem=xsend_sem.at[k], recv_sem=xrecv_sem.at[me],
            device_id=there, device_id_type=MESH))
        shares[-1].start()
    for k in range(1, devices):
        sender = (y + outer - k // inner) % outer * inner + (d + inner - k % inner) % inner
        pltpu.make_async_remote_copy(
            src_ref=xout, dst_ref=xin.at[sender], send_sem=xsend_sem.at[k], recv_sem=xrecv_sem.at[sender],
            device_id=partner, device_id_type=MESH).wait_recv()

    parts = xin[...]
    top = jnp.max(parts, axis=0)
    full = top + jnp.log(jnp.sum(jnp.exp(parts - top[None]), axis=0))
    positives = jnp.sum(parts, axis=0)[halves:halves + 1]
    total = jnp.sum(jnp.sum(full[:halves], axis=0, keepdims=True) - positives)
    mean_ref[0] = total / (devices * pairs)
    row = full[0:1]
    for h in range(1, halves):
        row = jnp.where(me // per_half == h, full[h:h + 1], row)
    row = pltpu.roll(row - own_row, (LANES - me % per_half * pairs) % LANES, 1)
    loss_ref[...] = row[:, :pairs]

    for send in sends + shares:
        send.wait_send()
    for i in range(1, chips):
        block_copy(me, relay_sem.at[i], partner).wait_send()


def solution(mesh):
    outer, inner = mesh.shape['data2'], mesh.shape['data']
    row_spec = P(('replica', 'data2', 'data'))
    tok_spec = P(('replica', 'data2', 'data'), None, None)
    mask_spec = P(('replica', 'data2', 'data'), None)

    def local_step(query_hidden, doc_hidden, w_proj, query_mask, doc_mask, temperature):
        pairs, qlen, hidden = query_hidden.shape
        dlen, width = doc_hidden.shape[1], w_proj.shape[1]
        devices, chips, tokens = outer * inner, outer * inner // CORES, pairs * qlen
        share_rows = -(-(devices * pairs // LANES + 1) // 4) * 4
        anywhere = pl.BlockSpec(memory_space=pltpu.HBM)
        vmem, dma = pltpu.VMEM, pltpu.SemaphoreType.DMA
        losses, mean_loss = pl.pallas_call(
            functools.partial(kernel, outer, inner, pairs, qlen, dlen),
            out_shape=(jax.ShapeDtypeStruct((1, pairs), jnp.float32), jax.ShapeDtypeStruct((1,), jnp.float32)),
            in_specs=[anywhere] * 5 + [pl.BlockSpec(memory_space=pltpu.SMEM)],
            out_specs=(pl.BlockSpec(memory_space=pltpu.VMEM), pl.BlockSpec(memory_space=pltpu.SMEM)),
            scratch_shapes=[
                vmem((tokens, hidden), jnp.bfloat16),
                vmem((pairs * dlen, hidden), jnp.bfloat16),
                vmem((hidden, width), jnp.bfloat16),
                vmem((pairs, qlen), jnp.int32),
                vmem((pairs, dlen), jnp.int32),
                vmem((devices, 2 * width, tokens), jnp.bfloat16),
                vmem((pairs * dlen, 2 * width), jnp.bfloat16),
                vmem((devices, pairs, tokens), jnp.float32),
                vmem((share_rows, LANES), jnp.float32),
                vmem((devices, share_rows, LANES), jnp.float32),
                dma((4,)), dma((DOC_CHUNKS,)), dma((chips,)), dma((chips,)), dma((devices,)),
                dma((devices,)), dma((devices,)),
            ],
            compiler_params=pltpu.CompilerParams(
                collective_id=0, has_side_effects=True, vmem_limit_bytes=67043328),
            name='late_interaction',
        )(query_hidden.reshape(tokens, hidden), doc_hidden.reshape(pairs * dlen, hidden), w_proj,
          query_mask, doc_mask, temperature.reshape(1))
        return losses.reshape(pairs), mean_loss

    return jax.shard_map(local_step, mesh=mesh,
                         in_specs=(tok_spec, tok_spec, P(None, None), mask_spec, mask_spec, P()),
                         out_specs=(row_spec, P('replica')), check_vma=False)
```
